32 devices in a mesh: row: 4 (over x, core), col: 4 (over z), head: 2 (over y).
Axes of the slice: x: 2, y: 2, z: 4, core: 2. Of those that a mesh axis runs over, the one named last changes fastest.
Arguments:
- query_map: bfloat16 [64, 128, 3072], P('row', 'col', 'head'), may hold values from -6 to 6
- key_map: bfloat16 [64, 128, 3072], P('row', 'col', 'head'), may hold values from -7 to 7
- value_map: bfloat16 [64, 128, 3072], P('row', 'col', 'head'), may hold values from -6 to 6
- window_mask: int32 [4, 4, 13, 13], P('row', 'col'), may hold values 0 or 1
- tile_radius: int32 [4, 4], P('row', 'col'), may hold values from 3 to 6, as said below
- dilation_per_tile: int32 [4, 4], P('row', 'col'), may hold values from 1 to 3, as said below
- rel_bias: float32 [48, 13, 13], P('head'), may hold values from -4 to 4
- out_weight: bfloat16 [3072, 3072], P('head'), may hold values from -0.109375 to 0.109375
Outputs:
- mixed: bfloat16 [64, 128, 3072], P('row', 'col', 'head')
The draws below stay inside these ranges and needn't reach their ends.
Inputs may be any that keep to these rules, and one draw needn't show every extreme that they name: `tile_radius`: in each row of tiles, at least one tile has radius 6 and dilation 3. `dilation_per_tile`: in each row of tiles, at least one tile has radius 6 and dilation 3.
All inputs are finite; a program needn't handle non-finite values. No bound on the sum of `window_mask` on one device may be relied on, other than what follows from the above.
Results may differ from the reference program's by a relative error of at most 0.0073.
Values may be sent and summed in bfloat16 or wider, within the bound.
No kernel may reach another device: no remote copies, remote signals or barrier semaphores. Data moves between devices by JAX's collectives and lax.ppermute only.
A program may use at most 384 MiB of HBM per device.

```python
import math
from functools import partial
import jax
import jax.numpy as jnp
from jax import lax

TILE_ROWS = 16
TILE_COLS = 32
HEADS = 48
HEAD_DIM = 64
RADIUS_MAX = 6
DILATION_LIMIT = 3
WINDOW = 13
HALO = 18
FEATURES = 3072
MODEL = 3072
ROWS = 64
COLS = 128
N_ROW = 4
N_COL = 4


def draw_query_map(key, part):
    drawn = jax.random.normal(jax.random.fold_in(key, 3), (ROWS, COLS, FEATURES), jnp.float32)
    return jnp.clip(drawn, -6.0, 6.0).astype(jnp.bfloat16)


def draw_key_map(key, part):
    drawn = jax.random.normal(jax.random.fold_in(key, 5), (ROWS, COLS, FEATURES), jnp.float32)
    return jnp.clip(drawn, -6.0, 6.0).astype(jnp.bfloat16)


def window_settings(key):
    base = jax.random.fold_in(key, 29)
    pick_key, radius_key, dilation_key = jax.random.split(base, 3)
    chosen_col = jax.random.randint(pick_key, (N_ROW,), 0, N_COL)
    radius = jax.random.randint(radius_key, (N_ROW, N_COL), 3, RADIUS_MAX + 1)
    dilation = jax.random.randint(dilation_key, (N_ROW, N_COL), 1, DILATION_LIMIT + 1)
    widest = jnp.arange(N_COL, dtype=jnp.int32)[None, :] == chosen_col[:, None]
    radius = jnp.where(widest, RADIUS_MAX, radius).astype(jnp.int32)
    dilation = jnp.where(widest, DILATION_LIMIT, dilation).astype(jnp.int32)
    return (radius, dilation)


def draw_tile_radius(key, part):
    return window_settings(key)[0]


def draw_dilation_per_tile(key, part):
    return window_settings(key)[1]


def touch_ends(result, own_key, smallest, top_value):
    index_at = [jax.random.randint(jax.random.fold_in(own_key, axis), (), 0, length) for axis, length in enumerate(result.shape)]
    longest = result.shape.index(max(result.shape))
    next_to = index_at[:longest] + [(index_at[longest] + 1) % result.shape[longest]] + index_at[longest + 1:]
    return result.at[tuple(index_at)].set(smallest).at[tuple(next_to)].set(top_value)


def shard_levels(key, shape, cuts, low, high):
    gain, own = 1.0, jax.random.fold_in(key, 6)
    for position, parts in cuts:
        draws = jnp.exp(jax.random.uniform(jax.random.fold_in(own, position), (parts,), jnp.float32, low / len(cuts), high / len(cuts)))
        gain = gain * jnp.repeat(draws, shape[position] // parts).reshape([-1 if axis == position else 1 for axis in range(len(shape))])
    return gain


def gaussian(rng, dims, width, limit, pieces=(), kind=jnp.bfloat16):
    values = width * jax.random.normal(rng, dims, jnp.float32)
    if pieces:
        values = values * shard_levels(rng, dims, pieces, -0.22, 0.18)
    return jnp.clip(values, -limit, limit).astype(kind)


def setup_inputs(seed: int = 0) -> dict:
    keys = jax.random.split(jax.random.key(seed), 9)
    query_map = draw_query_map(jax.random.fold_in(keys[8], 71), 0)
    key_map = draw_key_map(jax.random.fold_in(keys[8], 71), 0)
    value_map = gaussian(keys[2], (ROWS, COLS, FEATURES), 1.0, 6.0, ((0, 4), (1, 4), (2, 2)))
    window_mask = touch_ends((jax.random.randint(keys[3], (N_ROW, N_COL, WINDOW, WINDOW), 0, 4) < 3).astype(jnp.int32), jax.random.fold_in(keys[3], 1), 0, 1)
    tile_radius = draw_tile_radius(jax.random.fold_in(keys[8], 71), 0)
    dilation_per_tile = draw_dilation_per_tile(jax.random.fold_in(keys[8], 71), 0)
    rel_bias = gaussian(keys[6], (HEADS, WINDOW, WINDOW), 1.0, 4.0, ((0, 2),), jnp.float32)
    out_weight = gaussian(keys[7], (FEATURES, MODEL), FEATURES ** -0.5, 0.109375, ((0, 2),))
    return {"query_map": query_map, "key_map": key_map, "value_map": value_map, "window_mask": window_mask, "tile_radius": tile_radius, "dilation_per_tile": dilation_per_tile, "rel_bias": rel_bias, "out_weight": out_weight}


def tile_attention(index, query_map, padded_keys, padded_values, window_mask, tile_radius, dilation_per_tile, rel_bias):
    tile_row = index // N_COL
    tile_col = index % N_COL
    row_anchor = tile_row * TILE_ROWS
    col_anchor = tile_col * TILE_COLS
    zero_index = jnp.int32(0)
    queries = lax.dynamic_slice(query_map, (row_anchor, col_anchor, zero_index), (TILE_ROWS, TILE_COLS, FEATURES))
    queries = queries.astype(jnp.float32).reshape(TILE_ROWS, TILE_COLS, HEADS, HEAD_DIM)
    key_block = lax.dynamic_slice(padded_keys, (row_anchor, col_anchor, zero_index), (TILE_ROWS + 2 * HALO, TILE_COLS + 2 * HALO, FEATURES))
    value_block = lax.dynamic_slice(padded_values, (row_anchor, col_anchor, zero_index), (TILE_ROWS + 2 * HALO, TILE_COLS + 2 * HALO, FEATURES))
    radius = tile_radius[tile_row, tile_col]
    dilation = dilation_per_tile[tile_row, tile_col]
    pattern = window_mask[tile_row, tile_col]
    rows_here = row_anchor + jnp.arange(TILE_ROWS, dtype=jnp.int32)
    cols_here = col_anchor + jnp.arange(TILE_COLS, dtype=jnp.int32)
    score_scale = 1.0 / math.sqrt(HEAD_DIM)
    score_list = []
    mask_list = []
    starts = []
    for row_step in range(-RADIUS_MAX, RADIUS_MAX + 1):
        for col_step in range(-RADIUS_MAX, RADIUS_MAX + 1):
            row_start = HALO + row_step * dilation
            col_start = HALO + col_step * dilation
            starts.append((row_start, col_start))
            shifted = lax.dynamic_slice(key_block, (row_start, col_start, zero_index), (TILE_ROWS, TILE_COLS, FEATURES))
            shifted = shifted.astype(jnp.float32).reshape(TILE_ROWS, TILE_COLS, HEADS, HEAD_DIM)
            score = lax.optimization_barrier(jnp.sum(queries * shifted, axis=-1)) * score_scale
            score = score + rel_bias[:, row_step + RADIUS_MAX, col_step + RADIUS_MAX][None, None, :]
            inside = pattern[row_step + RADIUS_MAX, col_step + RADIUS_MAX] == 1
            if row_step == 0 and col_step == 0:
                inside = jnp.logical_or(inside, True)
            inside = inside & (abs(row_step) <= radius) & (abs(col_step) <= radius)
            row_global = rows_here + row_step * dilation
            col_global = cols_here + col_step * dilation
            row_fine = (row_global >= 0) & (row_global < ROWS)
            column_offset = (col_global >= 0) & (col_global < COLS)
            mask_list.append(inside & row_fine[:, None] & column_offset[None, :])
            score_list.append(score)
    scores = jnp.stack(score_list)
    masks = jnp.stack(mask_list)[..., None]
    peak_score = lax.optimization_barrier(jnp.max(jnp.where(masks, scores, -1e+30), axis=0, keepdims=True))
    exponent = jnp.where(masks, jnp.exp(jnp.where(masks, scores - peak_score, -60.0)), 0.0)
    denominator = lax.optimization_barrier(jnp.sum(exponent, axis=0, keepdims=True))
    weights = (exponent / denominator).astype(jnp.bfloat16)
    attended = jnp.zeros((TILE_ROWS, TILE_COLS, HEADS, HEAD_DIM), jnp.float32)
    for place in range(len(starts)):
        row_start, col_start = starts[place]
        shifted = lax.dynamic_slice(value_block, (row_start, col_start, zero_index), (TILE_ROWS, TILE_COLS, FEATURES))
        shifted = shifted.astype(jnp.float32).reshape(TILE_ROWS, TILE_COLS, HEADS, HEAD_DIM)
        attended = attended + weights[place].astype(jnp.float32)[..., None] * shifted
    return attended.reshape(TILE_ROWS, TILE_COLS, FEATURES).astype(jnp.bfloat16)

def reference(query_map, key_map, value_map, window_mask, tile_radius, dilation_per_tile, rel_bias, out_weight):
    padding = ((HALO, HALO), (HALO, HALO), (0, 0))
    padded_keys = jnp.pad(key_map, padding)
    padded_values = jnp.pad(value_map, padding)
    worker = partial(tile_attention, query_map=query_map, padded_keys=padded_keys, padded_values=padded_values, window_mask=window_mask, tile_radius=tile_radius, dilation_per_tile=dilation_per_tile, rel_bias=rel_bias)
    tiles = lax.map(worker, jnp.arange(N_ROW * N_COL, dtype=jnp.int32))
    tiles = tiles.reshape(N_ROW, N_COL, TILE_ROWS, TILE_COLS, FEATURES).transpose(0, 2, 1, 3, 4)
    attended = tiles.reshape(ROWS * COLS, FEATURES)
    mixed = jnp.dot(attended, out_weight, preferred_element_type=jnp.float32).astype(jnp.bfloat16)
    return mixed.reshape(ROWS, COLS, MODEL)
```

```python
import math

import jax
import jax.numpy as jnp
from jax import lax
from jax.experimental import pallas as pl
from jax.experimental.pallas import tpu as pltpu
from jax.sharding import PartitionSpec as P


HEAD_DIM = 64
RADIUS_MAX = 6
WINDOW = 13
HALO = 18
MASKED = -1e30
GROUP_HEADS = 4
GROUP_ROWS = 3
LAST_GROUPS = 1


def row_shift(value, steps):
    count = lax.axis_size("row")
    pairs = [(s, s + steps) for s in range(count) if 0 <= s + steps < count]
    return lax.ppermute(value, "row", pairs)


def col_shift_where(value, steps, row_ok):
    rows, cols = lax.axis_size("row"), lax.axis_size("col")
    pairs = [
        (r * cols + c, r * cols + c + steps)
        for r in range(rows)
        if row_ok(r)
        for c in range(cols)
        if 0 <= c + steps < cols
    ]
    return lax.ppermute(value, ("row", "col"), pairs)


def partner(value):
    count = lax.axis_size("row")
    return lax.ppermute(value, "row", [(s, s ^ 1) for s in range(count)])


def head_swap(value):
    return lax.ppermute(value, "head", [(0, 1), (1, 0)])


def head_partner(value):
    rows = lax.axis_size("row")
    pairs = [(2 * r + h, 2 * (r ^ 1) + 1 - h) for r in range(rows) for h in range(2)]
    return lax.ppermute(value, ("row", "head"), pairs)


def row_pair_swap(value):
    return lax.ppermute(value, "row", [(s, s ^ 2) for s in range(4)])


def tables_kernel(dims_ref, dims_row_ref, bias_ref, base_ref, *, slots):
    half = bias_ref.shape[0] // 2
    width = base_ref.shape[2]
    parity = dims_ref[2, 0]
    bias = jnp.where(parity == 0, bias_ref[:half], bias_ref[half:])
    index = lax.broadcasted_iota(jnp.int32, (1, WINDOW * WINDOW), 1)
    column = lax.broadcasted_iota(jnp.int32, (WINDOW * WINDOW, width), 0)
    lane = lax.broadcasted_iota(jnp.int32, (WINDOW * WINDOW, width), 1)
    for tile in range(2):
        radius, dilation = dims_ref[tile, 0], dims_ref[tile, 1]
        pattern = dims_row_ref[tile : tile + 1, 2:]
        up, side = index // WINDOW - RADIUS_MAX, index % WINDOW - RADIUS_MAX
        used = (jnp.abs(up) <= radius) & (jnp.abs(side) <= radius)
        used = used & ((pattern == 1) | ((up == 0) & (side == 0)))
        value = jnp.where(used, bias, MASKED)
        target = column // WINDOW * slots + (column % WINDOW - RADIUS_MAX) * dilation
        target = jnp.where(target < 0, target + width, target)
        spot = jnp.where(target == lane, 1.0, 0.0)
        placed = jnp.dot(value, spot, precision=lax.Precision.HIGHEST, preferred_element_type=jnp.float32)
        taken = jnp.max(spot, axis=0, keepdims=True)
        base_ref[tile] = jnp.where(taken > 0.0, placed, MASKED)


def tables(dims, bias, slots):
    half = bias.shape[0] // 2
    vmem = pl.BlockSpec(memory_space=pltpu.VMEM)

    def body(*refs):
        tables_kernel(*refs, slots=slots)

    return pl.pallas_call(
        body,
        out_shape=jax.ShapeDtypeStruct((2, half, (WINDOW + GROUP_ROWS) * slots), jnp.float32),
        in_specs=[pl.BlockSpec(memory_space=pltpu.SMEM), vmem, vmem],
        out_specs=vmem,
        name="tables",
    )(dims, dims, bias)


def give_half(parity, arrays):
    rows, cols, feats = arrays[0].shape
    half = feats // 2
    block = 4

    def body(parity_ref, *refs):
        for n, source in enumerate(refs[:-1]):
            refs[-1][n] = source[...]

    return pl.pallas_call(
        body,
        grid_spec=pltpu.PrefetchScalarGridSpec(
            num_scalar_prefetch=1,
            grid=(rows // block,),
            in_specs=[pl.BlockSpec((block, cols, half), lambda n, p: (n, 0, 1 - p[0]))] * len(arrays),
            out_specs=pl.BlockSpec((len(arrays), block, cols, half), lambda n, p: (0, n, 0, 0)),
        ),
        out_shape=jax.ShapeDtypeStruct((len(arrays), rows, cols, half), arrays[0].dtype),
        name="give_half",
    )(parity, *arrays)


def pack_kernel(flags_ref, key_ref, value_ref, recv_ref, *refs, low, edges):
    edge_refs, (right_ref, left_ref, mid_ref, sems) = refs[-4 - edges : -4], refs[-4:]
    rows, cols, half = recv_ref.shape[1:]
    feats = right_ref.shape[3]
    own_lanes = pl.ds(pl.multiple_of(flags_ref[0] * half + low, 256), feats)
    got_lanes = slice(low, low + feats)
    spill = HALO - rows

    def source(kv, own, *where):
        if own:
            return (key_ref, value_ref)[kv].at[(*where, own_lanes)]
        return recv_ref.at[(kv, *where, got_lanes)]

    made = []
    middles, others = [], []
    every = slice(None)
    for kv in range(2):
        for n, own in enumerate((True, False)):
            part = slice(n * rows, (n + 1) * rows)
            plans = [
                (source(kv, own, every, slice(cols // 2 - 8, cols // 2 + 8)), mid_ref.at[kv, part]),
                (source(kv, own, every, slice(cols - 16, cols)), right_ref.at[kv, part]),
                (source(kv, own, every, slice(0, 16)), left_ref.at[kv, part]),
            ]
            for index, (start, target) in enumerate(plans):
                copy = pltpu.make_async_copy(start, target, sems.at[len(made)])
                copy.start()
                made.append(copy)
                (others if index else middles).append(copy)
    sem0 = len(made)

    def edge_copies(n, own_near, downward):
        out_ref = edge_refs[n]
        copies = []
        for kv in range(2):
            far_rows = slice(rows - spill, rows) if downward else slice(0, spill)
            index = sem0 + 4 * n + 2 * kv
            copies.append(pltpu.make_async_copy(
                source(kv, own_near, every, every), out_ref.at[kv, 0:rows], sems.at[index]))
            copies.append(pltpu.make_async_copy(
                source(kv, not own_near, far_rows, every), out_ref.at[kv, rows:HALO], sems.at[index + 1]))
        return copies

    for n in range(edges):
        for code in range(4):
            own_near, downward = bool(code & 1), bool(code & 2)

            @pl.when(flags_ref[1 + n] == code)
            def _(n=n, own_near=own_near, downward=downward):
                for copy in edge_copies(n, own_near, downward):
                    copy.start()

    for copy in middles:
        copy.wait()
    for kv in range(2):
        for r in range(2 * rows):
            slot = r * 2
            spot = (kv, 2 * rows + slot // 16, slice(slot % 16, slot % 16 + 2))
            right_ref[spot] = mid_ref[kv, r, 6:8, :]
            left_ref[spot] = mid_ref[kv, r, 8:10, :]
    for copy in others:
        copy.wait()
    for n in range(edges):
        for copy in edge_copies(n, True, True):
            copy.wait()


def pack(flags, key_map, value_map, recv, low, feats, edges, after):
    _, rows, cols, _ = recv.shape
    hbm = pl.BlockSpec(memory_space=pl.ANY)
    vmem = pl.BlockSpec(memory_space=pltpu.VMEM)
    wire = jax.ShapeDtypeStruct((2, 2 * rows + 2 * rows * 2 // 16, 16, feats), recv.dtype)

    def body(*refs):
        pack_kernel(*refs, low=low, edges=edges)

    return pl.pallas_call(
        body,
        out_shape=[jax.ShapeDtypeStruct((2, HALO, cols, feats), recv.dtype)] * edges + [wire, wire],
        in_specs=[pl.BlockSpec(memory_space=pltpu.SMEM), hbm, hbm, hbm] + [hbm] * len(after),
        out_specs=[vmem] * (edges + 2),
        scratch_shapes=[
            pltpu.VMEM((2, 2 * rows, 16, feats), recv.dtype),
            pltpu.SemaphoreType.DMA((12 + 4 * edges,)),
        ],
        compiler_params=pltpu.CompilerParams(vmem_limit_bytes=40 * 1024 * 1024),
        name="pack",
    )(flags, key_map, value_map, recv, *after)


def pack_halo(middle, after):
    _, rows, cols, feats = middle.shape
    vmem = pl.BlockSpec(memory_space=pltpu.VMEM)
    tail = -(-rows * 2 // 16)
    wire = jax.ShapeDtypeStruct((2, rows + tail, 16, feats), middle.dtype)

    def body(in_ref, *refs):
        right_ref, left_ref = refs[-2:]
        for kv in range(2):
            right_ref[kv, 0:rows] = in_ref[kv, :, cols - 16 :, :]
            left_ref[kv, 0:rows] = in_ref[kv, :, 0:16, :]
            for ref in (right_ref, left_ref):
                ref[kv, rows + tail - 1] = jnp.zeros((16, feats), middle.dtype)
            for r in range(rows):
                slot = r * 2
                spot = (kv, rows + slot // 16, slice(slot % 16, slot % 16 + 2))
                right_ref[spot] = in_ref[kv, r, cols - HALO : cols - 16, :]
                left_ref[spot] = in_ref[kv, r, 16:HALO, :]

    return pl.pallas_call(
        body,
        out_shape=[wire, wire],
        in_specs=[vmem] + [pl.BlockSpec(memory_space=pl.ANY)] * len(after),
        out_specs=[vmem, vmem],
        compiler_params=pltpu.CompilerParams(vmem_limit_bytes=40 * 1024 * 1024),
        name="pack_halo",
    )(middle, *after)


def attend_kernel(meta_ref, base_ref, *refs, halos, low, total_cols):
    key_ref, value_ref, query_ref, recv_ref, side_right, side_left = refs[:6]
    halo_refs = refs[6 : 6 + 3 * halos]
    out_ref, slab_ref, q_ref, extra_ref, table_ref, rows_ref, sems = refs[-7:]
    groups, _, slab_rows, slots, feats = slab_ref.shape
    tile_rows, cols = q_ref.shape[2], q_ref.shape[3]
    half = recv_ref.shape[3]
    heads = feats // HEAD_DIM
    width = table_ref.shape[1]
    keys = (WINDOW + GROUP_ROWS - 1) * slots
    block = heads * cols
    own_row, other_row, pair_base, total_rows, own_off = [meta_ref[n] for n in (2, 3, 4, 5, 6)]
    parity, col_anchor = meta_ref[7], meta_ref[8]
    right_slots, extra_slots, left_slots = slice(cols, cols + 16), slice(cols + 16, cols + 32), slice(cols + 32, cols + 48)
    tail = 2 * tile_rows * 2 // 16
    halo_tail = -(-HALO * 2 // 16)

    def places(n):
        if n < 0:
            return [(own_off + own_row, tile_rows, 0), (own_off + other_row, tile_rows, tile_rows)]
        near, far = meta_ref[9 + 2 * n], meta_ref[10 + 2 * n]
        return [(near, tile_rows, 0), (far, HALO - tile_rows, tile_rows)]

    def copies(g):
        got = slice(low + g * feats, low + (g + 1) * feats)
        own = pl.ds(pl.multiple_of(parity * half + low + g * feats, feats), feats)
        here = slice(g * feats, (g + 1) * feats)
        made = []

        def add(source, target):
            made.append(pltpu.make_async_copy(source, target, sems.at[g, len(made)]))

        add(query_ref.at[:, :, own], q_ref.at[g, 0])
        add(recv_ref.at[2, :, :, got], q_ref.at[g, 1])
        for kv in range(2):
            slab = slab_ref.at[g, kv]
            add((key_ref, value_ref)[kv].at[:, :, own], slab.at[pl.ds(own_off + own_row, tile_rows), 0:cols])
            add(recv_ref.at[kv, :, :, got], slab.at[pl.ds(own_off + other_row, tile_rows), 0:cols])
            for n in range(-1, halos):
                if n < 0:
                    right, left, height, extra = side_right, side_left, 2 * tile_rows, 0
                else:
                    middle, right, left = halo_refs[3 * n : 3 * n + 3]
                    height, extra = HALO, tail + n * halo_tail
                for start, count, first in places(n):
                    rows = pl.ds(start, count)
                    part = slice(first, first + count)
                    if n >= 0:
                        add(middle.at[kv, part, :, here], slab.at[rows, 0:cols])
                    add(right.at[kv, part, :, here], slab.at[rows, right_slots])
                    add(left.at[kv, part, :, here], slab.at[rows, left_slots])
                count = tail if n < 0 else halo_tail
                for side, wire in enumerate((right, left)):
                    target = extra_ref.at[g, kv, side, extra : extra + count]
                    add(wire.at[kv, height : height + count, :, here], target)
        return made

    for g in range(groups):
        for copy in copies(g):
            copy.start()

    lane = lax.broadcasted_iota(jnp.int32, (1, width), 1)
    step = jnp.zeros((1, width), jnp.int32)
    for m in range(1, width // slots):
        step = step + jnp.where(lane >= m * slots, 1, 0)
    slot = lane - step * slots
    front_ok = jnp.where((slot < cols + HALO) & (col_anchor + slot < total_cols) & (lane < keys), 1, 0)
    back_ok = jnp.where((slot >= slots - HALO) & (col_anchor + slot >= slots) & (lane < keys), 2, 0)
    ok = jnp.broadcast_to(front_ok + back_ok, (cols, width))
    lane_head = lax.broadcasted_iota(jnp.int32, (cols, feats), 1) // HEAD_DIM
    scale = 1.0 / math.sqrt(HEAD_DIM)

    def fill_extras(g):
        for kv in range(2):
            slab_ref[g, kv, :, extra_slots, :] = jnp.zeros((slab_rows, 16, feats), jnp.bfloat16)
            for n in range(-1, halos):
                origin = 0 if n < 0 else tail + n * halo_tail
                for start, count, first in places(n):
                    for r in range(count):
                        at = (first + r) * 2
                        rows = slice(at % 16, at % 16 + 2)
                        where = origin + at // 16
                        slab_ref[g, kv, start + r, cols + 16 : cols + 18, :] = extra_ref[g, kv, 0, where, rows, :]
                        slab_ref[g, kv, start + r, cols + 30 : cols + 32, :] = extra_ref[g, kv, 1, where, rows, :]

    def one_tile(g, tile):
        dilation = meta_ref[tile]
        tile_row = meta_ref[2 + tile]
        for h in range(heads):
            base = jnp.broadcast_to(base_ref[tile, low // HEAD_DIM + g * heads + h][None, :], (cols, width))
            for n in range(GROUP_ROWS):
                front = pltpu.roll(base, n * slots, 1, stride=1, stride_axis=0)
                back = pltpu.roll(base, (n + 1) * slots, 1, stride=1, stride_axis=0)
                row0 = n * block + h * cols
                table_ref[row0 : row0 + cols, :] = jnp.where(
                    ok == 1, front, jnp.where(ok == 2, back, MASKED)
                )

        def unit(p, carry):
            first = (p // dilation) * (GROUP_ROWS * dilation) + p % dilation
            blocks = []
            for n in range(GROUP_ROWS):
                q_row = q_ref[g, tile, jnp.minimum(first + n * dilation, tile_rows - 1)]
                q_row = q_row.astype(jnp.float32) * scale
                blocks += [jnp.where(lane_head == h, q_row, 0.0).astype(jnp.bfloat16) for h in range(heads)]
            q_block = jnp.concatenate(blocks, axis=0)
            top = tile_row + first - RADIUS_MAX * dilation
            starts = [
                jnp.clip(own_off + top + m * dilation, 0, slab_rows - 1)
                for m in range(WINDOW + GROUP_ROWS - 1)
            ]
            k_rows = jnp.concatenate([slab_ref[g, 0, s] for s in starts], axis=0)
            v_rows = jnp.concatenate([slab_ref[g, 1, s] for s in starts], axis=0)
            scores = lax.dot_general(
                q_block, k_rows, (((1,), (1,)), ((), ())), preferred_element_type=jnp.float32
            )
            key_row = pair_base + top + step * dilation
            outside = jnp.where((key_row >= 0) & (key_row < total_rows), 0.0, MASKED)
            weights, sums = [], []
            for n in range(GROUP_ROWS):
                start = n * slots // 128 * 128
                stop = min(-(-(n + WINDOW) * slots // 128) * 128, keys)
                part = slice(n * block, (n + 1) * block)
                score = scores[part, start:stop] + table_ref[part, start:stop] + outside[:, start:stop]
                peak = jnp.max(score, axis=1, keepdims=True)
                exponent = jnp.exp(score - peak)
                sums.append(jnp.sum(exponent, axis=1, keepdims=True))
                pieces = [exponent.astype(jnp.bfloat16)]
                if start:
                    pieces.insert(0, jnp.zeros((block, start), jnp.bfloat16))
                if stop < keys:
                    pieces.append(jnp.zeros((block, keys - stop), jnp.bfloat16))
                weights.append(jnp.concatenate(pieces, axis=1))
            mixed = jnp.dot(
                jnp.concatenate(weights, axis=0), v_rows, preferred_element_type=jnp.float32
            ) / jnp.concatenate(sums, axis=0)
            for n in range(GROUP_ROWS):
                picked = mixed[n * block : n * block + cols]
                for h in range(1, heads):
                    row0 = n * block + h * cols
                    picked = jnp.where(lane_head == h, mixed[row0 : row0 + cols], picked)
                rows_ref[first + n * dilation] = picked.astype(jnp.bfloat16)
            return carry

        lax.fori_loop(0, -(-tile_rows // GROUP_ROWS), unit, 0, unroll=2)
        out_ref[tile, g] = rows_ref[0:tile_rows]

    for g in range(groups):
        for copy in copies(g):
            copy.wait()
        fill_extras(g)
        lax.fori_loop(0, 2, lambda tile, carry, g=g: (one_tile(g, tile), carry)[1], 0)


def attend(
    meta, base, key_map, value_map, query_map, recv, right, left, halos, after, low, all_feats, total_cols, slots
):
    _, tile_rows, cols, _ = recv.shape
    feats = GROUP_HEADS * HEAD_DIM
    groups = all_feats // feats
    slab_rows = 2 * tile_rows + HALO * len(halos)
    count = 2 * tile_rows * groups * GROUP_HEADS * cols * WINDOW * slots
    hbm = pl.BlockSpec(memory_space=pl.ANY)
    vmem = pl.BlockSpec(memory_space=pltpu.VMEM)
    flat = [array for halo in halos for array in halo] + list(after)
    tails = 2 * tile_rows * 2 // 16 + len(halos) * -(-HALO * 2 // 16)

    def body(*refs):
        attend_kernel(*refs, halos=len(halos), low=low, total_cols=total_cols)

    return pl.pallas_call(
        body,
        out_shape=jax.ShapeDtypeStruct((2, groups, tile_rows, cols, feats), jnp.bfloat16),
        in_specs=[pl.BlockSpec(memory_space=pltpu.SMEM), vmem] + [hbm] * (6 + len(flat)),
        out_specs=vmem,
        scratch_shapes=[
            pltpu.VMEM((groups, 2, slab_rows, slots, feats), jnp.bfloat16),
            pltpu.VMEM((groups, 2, tile_rows, cols, feats), jnp.bfloat16),
            pltpu.VMEM((groups, 2, 2, tails, 16, feats), jnp.bfloat16),
            pltpu.VMEM((GROUP_ROWS * GROUP_HEADS * cols, base.shape[2]), jnp.float32),
            pltpu.VMEM((tile_rows + 8, cols, feats), jnp.bfloat16),
            pltpu.SemaphoreType.DMA((groups, 2 + 2 * (8 + 8 * len(halos)))),
        ],
        compiler_params=pltpu.CompilerParams(vmem_limit_bytes=48 * 1024 * 1024),
        cost_estimate=pl.CostEstimate(
            flops=count * feats * 4, transcendentals=count, bytes_accessed=4 * groups * slab_rows * slots * feats
        ),
        name="attend",
    )(meta, base, key_map, value_map, query_map, recv, right, left, *flat)


def project(spots, pieces, out_weight, far_weights, low, half_feats, before, dtype):
    groups, tokens, feats = pieces[0].shape
    model = far_weights[0].shape[1]
    block = model // 3
    first = low // feats
    per_half = half_feats // feats
    columns = model // block
    whole = pl.BlockSpec((groups, tokens, feats), lambda n, spot: (0, 0, 0))
    column = pl.BlockSpec((tokens, block), lambda n, spot: (0, n))
    specs, arrays = [], []
    for source in range(4):
        for g in range(groups):
            if source < 2:

                def at(n, spot, source=source, g=g):
                    who = spot[0] if source == 0 else 1 - spot[0]
                    return who * per_half + first + g, spot[1] * columns + n

                arrays.append(out_weight)
            else:

                def at(n, spot, g=g):
                    return first + g, n

                arrays.append(far_weights[source - 2])
            specs.append(pl.BlockSpec((feats, block), at))
    extra = [] if before is None else [before]

    def body(spot_ref, *refs):
        lhs, rhs, out_ref = refs[:4], refs[4 : 4 + 4 * groups], refs[-1]
        total = refs[-2][...] if extra else None
        for source in range(4):
            for g in range(groups):
                term = jnp.dot(lhs[source][g], rhs[source * groups + g][...], preferred_element_type=jnp.float32)
                total = term if total is None else total + term
        out_ref[...] = total.astype(out_ref.dtype)

    return pl.pallas_call(
        body,
        grid_spec=pltpu.PrefetchScalarGridSpec(
            num_scalar_prefetch=1,
            grid=(columns,),
            in_specs=[whole] * 4 + specs + [column] * len(extra),
            out_specs=column,
        ),
        out_shape=jax.ShapeDtypeStruct((tokens, model), dtype),
        compiler_params=pltpu.CompilerParams(vmem_limit_bytes=40 * 1024 * 1024),
        cost_estimate=pl.CostEstimate(
            flops=8 * tokens * model * feats * groups,
            transcendentals=0,
            bytes_accessed=8 * model * feats * groups,
        ),
        name="project",
    )(spots, *pieces, *arrays, *extra)


def layer(
    query_map, key_map, value_map, window_mask, tile_radius, dilation_per_tile, rel_bias, out_weight
):
    tile_rows, tile_cols, features_dev = query_map.shape
    half_feats = features_dev // 2
    feats = GROUP_HEADS * HEAD_DIM
    slots = tile_cols + 48
    row_id = lax.axis_index("row")
    parity = row_id % 2
    pair_id = row_id // 2
    rows_count = lax.axis_size("row")
    pairs_count = rows_count // 2
    total_cols = tile_cols * lax.axis_size("col")
    tokens = tile_rows * tile_cols
    head_id = lax.axis_index("head")
    model_half = out_weight.shape[1] // 2

    given = give_half(parity.astype(jnp.int32)[None], (key_map, value_map, query_map))
    recv = partner(given)

    mine = jnp.concatenate([tile_radius[0], dilation_per_tile[0], window_mask[0, 0].reshape(-1)])
    others = partner(mine)
    who = jnp.full_like(mine, parity)
    dims = jnp.stack([mine, others, who])
    base = tables(dims, rel_bias.reshape(rel_bias.shape[0], -1), slots)

    spill = HALO - tile_rows
    pair_rows = 2 * tile_rows
    first_pair = pair_id == 0
    if pairs_count == 1:
        own_off, spots, downs = 0, [], []
    elif pairs_count == 2:
        own_off = jnp.where(first_pair, 0, HALO)
        spots = [jnp.where(first_pair, pair_rows, spill), jnp.where(first_pair, pair_rows + tile_rows, 0)]
        downs = [first_pair.astype(jnp.int32)]
    else:
        own_off = HALO
        spots = [spill, 0, HALO + pair_rows, HALO + pair_rows + tile_rows]
        downs = [1, 0]
    meta = [dims[0, 1], dims[1, 1], parity * tile_rows, (1 - parity) * tile_rows]
    meta += [pair_id * pair_rows, tile_rows * rows_count, own_off, parity]
    meta += [lax.axis_index("col") * tile_cols, *spots]
    meta = jnp.stack([jnp.asarray(item, jnp.int32) for item in meta])
    flags = [parity] + [2 * down + jnp.where(parity == down, 1, 0) for down in downs]
    flags = jnp.stack([jnp.asarray(item, jnp.int32) for item in flags])

    total_groups = half_feats // feats
    spans = [(0, total_groups - LAST_GROUPS), (total_groups - LAST_GROUPS, total_groups)]
    packs, after = [], []
    for low, high in spans:
        packed = pack(
            flags, key_map, value_map, recv, low * feats, (high - low) * feats, len(downs), after
        )
        after = [packed[-1]]
        packs.append(packed)
    ready = []
    for *edges, right, left in packs:
        middles = []
        if pairs_count == 2:
            middles = [(row_pair_swap(edges[0]), lambda r: True)]
        elif pairs_count > 2:
            middles = [
                (row_shift(edges[0], 2), lambda r: r >= 2),
                (row_shift(edges[1], -2), lambda r: r < rows_count - 2),
            ]
        left_in = col_shift_where(right, 1, lambda r: True)
        right_in = col_shift_where(left, -1, lambda r: True)
        halos = []
        for middle, row_ok in middles:
            right_out, left_out = pack_halo(middle, after)
            after = [left_out]
            halos.append(
                (middle, col_shift_where(left_out, -1, row_ok), col_shift_where(right_out, 1, row_ok))
            )
        ready.append((right_in, left_in, halos))

    give = lax.dynamic_slice(out_weight, (parity * half_feats, (1 - head_id) * model_half), (half_feats, model_half))
    far_weight = head_swap(give)
    corner = jnp.stack([parity, head_id]).astype(jnp.int32)

    exchanged = []
    for (low, high), (right_in, left_in, halos) in zip(spans, ready):
        done = attend(
            meta, base, key_map, value_map, query_map, recv, right_in, left_in, halos, after,
            low * feats, (high - low) * feats, total_cols, slots,
        )
        if not exchanged:
            far_weights = [far_weight, partner(lax.optimization_barrier((far_weight, done))[0])]
        after = [done]
        own, other = done[0], done[1]
        pieces = [own, partner(other), head_swap(own), head_partner(other)]
        exchanged.append([piece.reshape(high - low, tokens, feats) for piece in pieces])
    acc = None
    for (low, high), pieces in zip(spans, exchanged):
        dtype = jnp.bfloat16 if high == total_groups else jnp.float32
        acc = project(corner, pieces, out_weight, far_weights, low * feats, half_feats, acc, dtype)
    return acc.reshape(tile_rows, tile_cols, model_half)


def solution(mesh):
    placed = (
        P("row", "col", "head"),
        P("row", "col", "head"),
        P("row", "col", "head"),
        P("row", "col", None, None),
        P("row", "col"),
        P("row", "col"),
        P("head", None, None),
        P("head", None),
    )
    return jax.shard_map(layer, mesh=mesh, in_specs=placed, out_specs=P("row", "col", "head"), check_vma=False)
```

```python
import math

import jax
import jax.numpy as jnp
from jax import lax
from jax.experimental import pallas as pl
from jax.experimental.pallas import tpu as pltpu
from jax.sharding import PartitionSpec as P


HEAD_DIM = 64
RADIUS_MAX = 6
WINDOW = 13
HALO = 18
MASKED = -1e30
GROUP_HEADS = 4
GROUP_ROWS = 3


def row_shift(value, steps):
    count = lax.axis_size("row")
    pairs = [(s, s + steps) for s in range(count) if 0 <= s + steps < count]
    return lax.ppermute(value, "row", pairs)


def col_swap_where(value, odd, row_ok):
    rows, cols = lax.axis_size("row"), lax.axis_size("col")
    pairs = []
    for r in range(rows):
        for c in range(odd, cols - 1, 2):
            if row_ok(r):
                low = r * cols + c
                pairs += [(low, low + 1), (low + 1, low)]
    return lax.ppermute(value, ("row", "col"), pairs)


def partner(value):
    count = lax.axis_size("row")
    return lax.ppermute(value, "row", [(s, s ^ 1) for s in range(count)])


def head_swap(value):
    return lax.ppermute(value, "head", [(0, 1), (1, 0)])


def head_partner(value):
    rows = lax.axis_size("row")
    pairs = [(2 * r + h, 2 * (r ^ 1) + 1 - h) for r in range(rows) for h in range(2)]
    return lax.ppermute(value, ("row", "head"), pairs)


def row_pair_swap(value):
    return lax.ppermute(value, "row", [(s, s ^ 2) for s in range(4)])


def tables_kernel(dims_ref, dims_row_ref, bias_ref, base_ref, *, slots):
    half = bias_ref.shape[0] // 2
    width = base_ref.shape[2]
    parity = lax.axis_index("row") % 2
    bias = jnp.where(parity == 0, bias_ref[:half], bias_ref[half:])
    index = lax.broadcasted_iota(jnp.int32, (1, WINDOW * WINDOW), 1)
    column = lax.broadcasted_iota(jnp.int32, (WINDOW * WINDOW, width), 0)
    lane = lax.broadcasted_iota(jnp.int32, (WINDOW * WINDOW, width), 1)
    for tile in range(2):
        radius, dilation = dims_ref[tile, 0], dims_ref[tile, 1]
        pattern = dims_row_ref[tile : tile + 1, 2:]
        up, side = index // WINDOW - RADIUS_MAX, index % WINDOW - RADIUS_MAX
        used = (jnp.abs(up) <= radius) & (jnp.abs(side) <= radius)
        used = used & ((pattern == 1) | ((up == 0) & (side == 0)))
        value = jnp.where(used, bias, MASKED)
        target = column // WINDOW * slots + (column % WINDOW - RADIUS_MAX) * dilation
        target = jnp.where(target < 0, target + width, target)
        spot = jnp.where(target == lane, 1.0, 0.0)
        placed = jnp.dot(value, spot, precision=lax.Precision.HIGHEST, preferred_element_type=jnp.float32)
        taken = jnp.max(spot, axis=0, keepdims=True)
        base_ref[tile] = jnp.where(taken > 0.0, placed, MASKED)


def tables(dims, bias, slots):
    half = bias.shape[0] // 2
    vmem = pl.BlockSpec(memory_space=pltpu.VMEM)

    def body(*refs):
        tables_kernel(*refs, slots=slots)

    return pl.pallas_call(
        body,
        out_shape=jax.ShapeDtypeStruct((2, half, (WINDOW + GROUP_ROWS) * slots), jnp.float32),
        in_specs=[pl.BlockSpec(memory_space=pltpu.SMEM), vmem, vmem],
        out_specs=vmem,
        name="tables",
    )(dims, dims, bias)


def give_half(parity, parts, feats):
    rows, cols, all_feats = parts[0][0].shape
    per_half = all_feats // 2 // feats
    block = 8

    def body(parity_ref, *refs):
        for n, source in enumerate(refs[:-1]):
            refs[-1][n] = source[...]

    def spec(chunk):
        return pl.BlockSpec((block, cols, feats), lambda n, p: (n, 0, (1 - p[0]) * per_half + chunk))

    return pl.pallas_call(
        body,
        grid_spec=pltpu.PrefetchScalarGridSpec(
            num_scalar_prefetch=1,
            grid=(rows // block,),
            in_specs=[spec(chunk) for _, chunk in parts],
            out_specs=pl.BlockSpec((len(parts), block, cols, feats), lambda n, p: (0, n, 0, 0)),
        ),
        out_shape=jax.ShapeDtypeStruct((len(parts), rows, cols, feats), parts[0][0].dtype),
        name="give_half",
    )(parity, *[array for array, _ in parts])


def place():
    row = lax.axis_index("row")
    return row % 2, row // 2, lax.axis_index("col") % 2


def send_out(sources, targets, sems, swap):
    for flip in range(2):

        @pl.when(swap == flip)
        def _(flip=flip):
            made = [
                pltpu.make_async_copy(source, targets[n ^ flip], sems[n]) for n, source in enumerate(sources)
            ]
            for copy in made:
                copy.start()
            for copy in made:
                copy.wait()


def pack_kernel(key_ref, value_ref, recv_ref, *refs, low, downs, edge_lows, halos, wires):
    edges = len(downs) * len(edge_lows)
    rows, cols = recv_ref.shape[1:3]
    half = key_ref.shape[2] // 2
    middle_refs = refs[:halos]
    out_refs, (right_ref, left_ref, mid_ref, edge_ref, sems) = refs[-5 - edges - 2 * wires : -5], refs[-5:]
    edge_outs, wire_outs = out_refs[:edges], out_refs[edges:]
    feats = right_ref.shape[3]
    parity, pair, col_parity = place()
    spill = HALO - rows
    every = slice(None)

    def source(kv, own, start, *where):
        if own:
            lanes = pl.ds(pl.multiple_of(parity * half + start, feats), feats)
            return (key_ref, value_ref)[kv].at[(*where, lanes)]
        return recv_ref.at[(2 * (start // feats) + kv, *where, every)]

    count = 0
    middles, others = [], []

    def start_copy(begin, target, group):
        nonlocal count
        copy = pltpu.make_async_copy(begin, target, sems.at[count])
        count += 1
        copy.start()
        group.append(copy)

    def columns(begin, part, top):
        height = part.stop - part.start
        for kv in range(2):
            start_copy(begin(kv, slice(cols // 2 - 8, cols // 2 + 8)), mid_ref.at[kv, part], middles)
            body = slice(top, top + height)
            start_copy(begin(kv, slice(cols - 16, cols)), right_ref.at[kv, body], others)
            start_copy(begin(kv, slice(0, 16)), left_ref.at[kv, body], others)

    if wires:
        for n, own in enumerate((True, False)):
            part = slice(n * rows, (n + 1) * rows)
            columns(lambda kv, at, own=own: source(kv, own, low, every, at), part, n * rows)
        for n, middle in enumerate(middle_refs):
            part = slice(2 * rows + n * HALO, 2 * rows + (n + 1) * HALO)
            top = wire_rows(2 * rows) + n * wire_rows(HALO)
            columns(lambda kv, at, middle=middle: middle.at[kv, :, at], part, top)

    def edge_copies(chunk, n, own_near, downward):
        copies = []
        spot = chunk * len(downs) + n
        for kv in range(2):
            far_rows = slice(rows - spill, rows) if downward else slice(0, spill)
            index = count + 4 * spot + 2 * kv
            near, far = edge_ref.at[spot, kv, 0:rows], edge_ref.at[spot, kv, rows:HALO]
            begin = edge_lows[chunk]
            near_from = source(kv, own_near, begin, every, every)
            far_from = source(kv, not own_near, begin, far_rows, every)
            copies.append(pltpu.make_async_copy(near_from, near, sems.at[index]))
            copies.append(pltpu.make_async_copy(far_from, far, sems.at[index + 1]))
        return copies

    for n, down in enumerate(downs if edge_lows else []):
        goes_down = jnp.where(pair == 0, 1, 0) if down is None else down
        code = jnp.where(parity == goes_down, 1, 0) + 2 * goes_down
        for case in range(4):

            @pl.when(code == case)
            def _(n=n, case=case):
                for chunk in range(len(edge_lows)):
                    for copy in edge_copies(chunk, n, bool(case & 1), bool(case & 2)):
                        copy.start()

    def pair_up(first, height, top):
        for kv in range(2):
            if height * 2 % 16:
                for ref in (right_ref, left_ref):
                    ref[kv, top + wire_rows(height) - 1] = jnp.zeros((16, feats), recv_ref.dtype)
            for r in range(height):
                slot = r * 2
                spot = (kv, top + height + slot // 16, slice(slot % 16, slot % 16 + 2))
                right_ref[spot] = mid_ref[kv, first + r, 6:8, :]
                left_ref[spot] = mid_ref[kv, first + r, 8:10, :]

    sent = []
    if edge_lows:
        for chunk in range(len(edge_lows)):
            for n in range(len(downs)):
                for copy in edge_copies(chunk, n, True, True):
                    copy.wait()
        for n in range(edges):
            sent.append(pltpu.make_async_copy(edge_ref.at[n], edge_outs[n], sems.at[count + 4 * edges + n]))
            sent[-1].start()
    if wires:
        for copy in middles:
            copy.wait()
        pair_up(0, 2 * rows, 0)
        for n in range(halos):
            pair_up(2 * rows + n * HALO, HALO, wire_rows(2 * rows) + n * wire_rows(HALO))
        for copy in others:
            copy.wait()
        last = count + 5 * edges
        send_out([right_ref, left_ref], wire_outs, [sems.at[last], sems.at[last + 1]], col_parity)
    for copy in sent:
        copy.wait()


def wire_rows(height):
    return height + -(-height * (HALO - 16) // 16)


def pack(key_map, value_map, recv, low, feats, downs, edge_lows, middles, wires, after):
    _, rows, cols, _ = recv.shape
    edges, halos = len(downs) * len(edge_lows), len(middles)
    hbm = pl.BlockSpec(memory_space=pltpu.HBM)
    height = wire_rows(2 * rows) + halos * wire_rows(HALO)
    wire = jax.ShapeDtypeStruct((2, height, 16, feats), recv.dtype)

    def body(*refs):
        pack_kernel(*refs, low=low, downs=downs, edge_lows=edge_lows, halos=halos, wires=wires)

    return pl.pallas_call(
        body,
        out_shape=[jax.ShapeDtypeStruct((2, HALO, cols, feats), recv.dtype)] * edges + [wire, wire] * wires,
        in_specs=[hbm] * (3 + halos + len(after)),
        out_specs=[hbm] * (edges + 2 * wires),
        scratch_shapes=[
            pltpu.VMEM((2, height, 16, feats), recv.dtype),
            pltpu.VMEM((2, height, 16, feats), recv.dtype),
            pltpu.VMEM((2, 2 * rows + halos * HALO, 16, feats), recv.dtype),
            pltpu.VMEM((max(edges, 1), 2, HALO, cols, feats), recv.dtype),
            pltpu.SemaphoreType.DMA((14 + 6 * halos + 5 * edges,)),
        ],
        compiler_params=pltpu.CompilerParams(vmem_limit_bytes=40 * 1024 * 1024),
        name="pack",
    )(key_map, value_map, recv, *middles, *after)


def pack_halo(middle, after):
    _, rows, cols, feats = middle.shape
    vmem = pl.BlockSpec(memory_space=pltpu.VMEM)
    hbm = pl.BlockSpec(memory_space=pltpu.HBM)
    height = wire_rows(rows)
    tail = height - rows
    wire = jax.ShapeDtypeStruct((2, height, 16, feats), middle.dtype)

    def body(in_ref, *refs):
        first_out, second_out, right_ref, left_ref, sems = refs[-5:]
        for kv in range(2):
            right_ref[kv, 0:rows] = in_ref[kv, :, cols - 16 :, :]
            left_ref[kv, 0:rows] = in_ref[kv, :, 0:16, :]
            for ref in (right_ref, left_ref):
                ref[kv, rows + tail - 1] = jnp.zeros((16, feats), middle.dtype)
            for r in range(rows):
                slot = r * 2
                spot = (kv, rows + slot // 16, slice(slot % 16, slot % 16 + 2))
                right_ref[spot] = in_ref[kv, r, cols - HALO : cols - 16, :]
                left_ref[spot] = in_ref[kv, r, 16:HALO, :]
        send_out([right_ref, left_ref], [first_out, second_out], [sems.at[0], sems.at[1]], place()[2])

    return pl.pallas_call(
        body,
        out_shape=[wire, wire],
        in_specs=[vmem] + [hbm] * len(after),
        out_specs=[hbm, hbm],
        scratch_shapes=[pltpu.VMEM(wire.shape, wire.dtype)] * 2 + [pltpu.SemaphoreType.DMA((2,))],
        compiler_params=pltpu.CompilerParams(vmem_limit_bytes=40 * 1024 * 1024),
        name="pack_halo",
    )(middle, *after)


def attend_kernel(dims_ref, base_ref, *refs, halos, joined, low, tiles, recv_at, query_at):
    key_ref, value_ref, query_ref, recv_ref, side_first, side_second = refs[:6]
    per_halo = 1 if joined else 3
    halo_refs = refs[6 : 6 + per_halo * halos]
    out_ref, slab_ref, q_ref, extra_ref, table_ref, rows_ref, sems = refs[-7:]
    groups, _, slab_rows, slots, feats = slab_ref.shape
    tile_rows, cols = q_ref.shape[2], q_ref.shape[3]
    half = key_ref.shape[2] // 2
    heads = feats // HEAD_DIM
    width = table_ref.shape[1]
    keys = (WINDOW + GROUP_ROWS - 1) * slots
    block = heads * cols
    parity, pair, col_parity = place()
    own_row, other_row = parity * tile_rows, (1 - parity) * tile_rows
    spill, pair_rows = HALO - tile_rows, 2 * tile_rows
    pair_base = pair * pair_rows
    total_rows = tile_rows * lax.axis_size("row")
    total_cols = cols * lax.axis_size("col")
    col_anchor = lax.axis_index("col") * cols
    if halos == 0:
        own_off, spots = 0, []
    elif halos == 1:
        own_off = jnp.where(pair == 0, 0, HALO)
        spots = [(jnp.where(pair == 0, pair_rows, spill), jnp.where(pair == 0, pair_rows + tile_rows, 0))]
    else:
        own_off = HALO
        spots = [(spill, 0), (HALO + pair_rows, HALO + pair_rows + tile_rows)]
    slots_at = [cols + 32 * col_parity, cols + 32 * (1 - col_parity)]
    slots_at = [pl.ds(pl.multiple_of(at, 16), 16) for at in slots_at]
    sides_at = [col_parity, 1 - col_parity]
    extra_slots = slice(cols + 16, cols + 32)
    tail = 2 * tile_rows * 2 // 16
    halo_tail = -(-HALO * 2 // 16)

    def places(n):
        if n < 0:
            return [(own_off + own_row, tile_rows, 0), (own_off + other_row, tile_rows, tile_rows)]
        near, far = spots[n]
        return [(near, tile_rows, 0), (far, HALO - tile_rows, tile_rows)]

    def copies(g):
        own = pl.ds(pl.multiple_of(parity * half + low + g * feats, feats), feats)
        here = pl.ds(pl.multiple_of(g * feats, feats), feats)
        made = []

        def add(source, target):
            made.append(pltpu.make_async_copy(source, target, sems.at[g, len(made)]))

        add(query_ref.at[:, :, own], q_ref.at[g, 0])
        add(recv_ref.at[query_at], q_ref.at[g, 1])
        for kv in range(2):
            slab = slab_ref.at[g, kv]
            add((key_ref, value_ref)[kv].at[:, :, own], slab.at[pl.ds(own_off + own_row, tile_rows), 0:cols])
            add(recv_ref.at[recv_at + kv], slab.at[pl.ds(own_off + other_row, tile_rows), 0:cols])
            for n in range(-1, halos):
                wires, top, height, extra = (side_first, side_second), 0, 2 * tile_rows, 0
                if n >= 0:
                    height, extra = HALO, tail + n * halo_tail
                    middle = halo_refs[per_halo * n]
                    if joined:
                        top = wire_rows(2 * tile_rows) + n * wire_rows(HALO)
                    else:
                        wires = halo_refs[3 * n + 1 : 3 * n + 3]
                for start, count, first in places(n):
                    rows = pl.ds(start, count)
                    if n >= 0:
                        add(middle.at[kv, first : first + count, :, here], slab.at[rows, 0:cols])
                    part = slice(top + first, top + first + count)
                    for wire, at in zip(wires, slots_at):
                        add(wire.at[kv, part, :, here], slab.at[rows, at])
                count = tail if n < 0 else halo_tail
                for side, wire in zip(sides_at, wires):
                    target = extra_ref.at[g, kv, side, extra : extra + count]
                    add(wire.at[kv, top + height : top + height + count, :, here], target)
        return made

    def start_group(g, carry):
        for copy in copies(g):
            copy.start()
        return carry

    lax.fori_loop(0, groups, start_group, 0)

    lane = lax.broadcasted_iota(jnp.int32, (1, width), 1)
    step = jnp.zeros((1, width), jnp.int32)
    for m in range(1, width // slots):
        step = step + jnp.where(lane >= m * slots, 1, 0)
    slot = lane - step * slots
    front_ok = jnp.where((slot < cols + HALO) & (col_anchor + slot < total_cols) & (lane < keys), 1, 0)
    back_ok = jnp.where((slot >= slots - HALO) & (col_anchor + slot >= slots) & (lane < keys), 2, 0)
    ok = jnp.broadcast_to(front_ok + back_ok, (cols, width))
    lane_head = lax.broadcasted_iota(jnp.int32, (cols, feats), 1) // HEAD_DIM
    scale = 1.0 / math.sqrt(HEAD_DIM)

    def fill_extras(g):
        for kv in range(2):
            slab_ref[g, kv, :, extra_slots, :] = jnp.zeros((slab_rows, 16, feats), jnp.bfloat16)
            for n in range(-1, halos):
                origin = 0 if n < 0 else tail + n * halo_tail
                for start, count, first in places(n):
                    for r in range(count):
                        at = (first + r) * 2
                        rows = slice(at % 16, at % 16 + 2)
                        where = origin + at // 16
                        slab_ref[g, kv, start + r, cols + 16 : cols + 18, :] = extra_ref[g, kv, 0, where, rows, :]
                        slab_ref[g, kv, start + r, cols + 30 : cols + 32, :] = extra_ref[g, kv, 1, where, rows, :]

    def fill_table(g, tile):
        for h in range(heads):
            head = low // HEAD_DIM + g * heads + h
            base = jnp.broadcast_to(base_ref[tile, pl.ds(head, 1), :], (cols, width))
            for n in range(GROUP_ROWS):
                front = pltpu.roll(base, n * slots, 1, stride=1, stride_axis=0)
                back = pltpu.roll(base, (n + 1) * slots, 1, stride=1, stride_axis=0)
                row0 = n * block + h * cols
                table_ref[row0 : row0 + cols, :] = jnp.where(
                    ok == 1, front, jnp.where(ok == 2, back, MASKED)
                )

    def one_tile(g, tile):
        dilation = dims_ref[tile, 1]
        tile_row = jnp.where(tile == 0, own_row, other_row)

        def unit(p, carry):
            first = (p // dilation) * (GROUP_ROWS * dilation) + p % dilation
            blocks = []
            for n in range(GROUP_ROWS):
                q_row = q_ref[g, tile, jnp.minimum(first + n * dilation, tile_rows - 1)]
                q_row = q_row.astype(jnp.float32) * scale
                blocks += [jnp.where(lane_head == h, q_row, 0.0).astype(jnp.bfloat16) for h in range(heads)]
            q_block = jnp.concatenate(blocks, axis=0)
            top = tile_row + first - RADIUS_MAX * dilation
            starts = [
                jnp.clip(own_off + top + m * dilation, 0, slab_rows - 1)
                for m in range(WINDOW + GROUP_ROWS - 1)
            ]
            k_rows = jnp.concatenate([slab_ref[g, 0, s] for s in starts], axis=0)
            v_rows = jnp.concatenate([slab_ref[g, 1, s] for s in starts], axis=0)
            scores = lax.dot_general(
                q_block, k_rows, (((1,), (1,)), ((), ())), preferred_element_type=jnp.float32
            )
            key_row = pair_base + top + step * dilation
            outside = jnp.where((key_row >= 0) & (key_row < total_rows), 0.0, MASKED)
            weights, sums = [], []
            for n in range(GROUP_ROWS):
                start = n * slots // 128 * 128
                stop = min(-(-(n + WINDOW) * slots // 128) * 128, keys)
                part = slice(n * block, (n + 1) * block)
                score = scores[part, start:stop] + table_ref[part, start:stop] + outside[:, start:stop]
                peak = jnp.max(score, axis=1, keepdims=True)
                exponent = jnp.exp(score - peak)
                sums.append(jnp.sum(exponent, axis=1, keepdims=True))
                pieces = [exponent.astype(jnp.bfloat16)]
                if start:
                    pieces.insert(0, jnp.zeros((block, start), jnp.bfloat16))
                if stop < keys:
                    pieces.append(jnp.zeros((block, keys - stop), jnp.bfloat16))
                weights.append(jnp.concatenate(pieces, axis=1))
            mixed = jnp.dot(
                jnp.concatenate(weights, axis=0), v_rows, preferred_element_type=jnp.float32
            ) / jnp.concatenate(sums, axis=0)
            for n in range(GROUP_ROWS):
                picked = mixed[n * block : n * block + cols]
                for h in range(1, heads):
                    row0 = n * block + h * cols
                    picked = jnp.where(lane_head == h, mixed[row0 : row0 + cols], picked)
                rows_ref[first + n * dilation] = picked.astype(jnp.bfloat16)
            return carry

        lax.fori_loop(0, -(-tile_rows // GROUP_ROWS), unit, 0, unroll=True)
        out_ref[tile - tiles[0], g] = rows_ref[0:tile_rows]

    def one_group(g, carry):
        fill_table(g, tiles[0])
        for copy in copies(g):
            copy.wait()
        fill_extras(g)

        def tile_step(tile, inner):
            @pl.when(tile > tiles[0])
            def _():
                fill_table(g, tile)

            one_tile(g, tile)
            return inner

        lax.fori_loop(tiles[0], tiles[-1] + 1, tile_step, 0)
        return carry

    lax.fori_loop(0, groups, one_group, 0)


def attend(
    dims, base, key_map, value_map, query_map, recv, first, second, halos, joined, after,
    low, all_feats, slots, tiles, recv_at, query_at,
):
    _, tile_rows, cols, _ = recv.shape
    feats = GROUP_HEADS * HEAD_DIM
    groups = all_feats // feats
    slab_rows = 2 * tile_rows + HALO * len(halos)
    count = len(tiles) * tile_rows * groups * GROUP_HEADS * cols * WINDOW * slots
    hbm = pl.BlockSpec(memory_space=pltpu.HBM)
    vmem = pl.BlockSpec(memory_space=pltpu.VMEM)
    flat = [array for halo in halos for array in halo] + list(after)
    tails = 2 * tile_rows * 2 // 16 + len(halos) * -(-HALO * 2 // 16)

    def body(*refs):
        attend_kernel(*refs, halos=len(halos), joined=joined, low=low, tiles=tiles, recv_at=recv_at, query_at=query_at)

    return pl.pallas_call(
        body,
        out_shape=jax.ShapeDtypeStruct((len(tiles), groups, tile_rows, cols, feats), jnp.bfloat16),
        in_specs=[pl.BlockSpec(memory_space=pltpu.SMEM), vmem] + [hbm] * (6 + len(flat)),
        out_specs=vmem,
        scratch_shapes=[
            pltpu.VMEM((groups, 2, slab_rows, slots, feats), jnp.bfloat16),
            pltpu.VMEM((groups, 2, tile_rows, cols, feats), jnp.bfloat16),
            pltpu.VMEM((groups, 2, 2, tails, 16, feats), jnp.bfloat16),
            pltpu.VMEM((GROUP_ROWS * GROUP_HEADS * cols, base.shape[2]), jnp.float32),
            pltpu.VMEM((tile_rows + 8, cols, feats), jnp.bfloat16),
            pltpu.SemaphoreType.DMA((groups, 2 + 2 * (8 + 8 * len(halos)))),
        ],
        compiler_params=pltpu.CompilerParams(vmem_limit_bytes=48 * 1024 * 1024),
        cost_estimate=pl.CostEstimate(
            flops=count * feats * 4, transcendentals=count, bytes_accessed=4 * groups * slab_rows * slots * feats
        ),
        name="attend",
    )(dims, base, key_map, value_map, query_map, recv, first, second, *flat)


def project(spots, terms, out_weight, far_weights, half_feats, before, dtype):
    tokens, feats = terms[0][2].shape
    model = far_weights[0].shape[1]
    block = model // 3
    per_half = half_feats // feats
    columns = model // block
    whole = pl.BlockSpec((tokens, feats), lambda n, spot: (0, 0))
    column = pl.BlockSpec((tokens, block), lambda n, spot: (0, n))
    specs, arrays, pieces = [], [], []
    for index, source, piece in terms:
        if source < 2:

            def at(n, spot, source=source, index=index):
                who = spot[0] if source == 0 else 1 - spot[0]
                return who * per_half + index, spot[1] * columns + n

            arrays.append(out_weight)
        else:

            def at(n, spot, index=index):
                return index, n

            arrays.append(far_weights[source - 2])
        pieces.append(piece)
        specs.append(pl.BlockSpec((feats, block), at))
    extra = [] if before is None else [before]
    count = len(pieces)

    def body(spot_ref, *refs):
        total = refs[-2][...] if extra else None
        for lhs, rhs in zip(refs[:count], refs[count : 2 * count]):
            term = jnp.dot(lhs[...], rhs[...], preferred_element_type=jnp.float32)
            total = term if total is None else total + term
        refs[-1][...] = total.astype(dtype)

    return pl.pallas_call(
        body,
        grid_spec=pltpu.PrefetchScalarGridSpec(
            num_scalar_prefetch=1,
            grid=(columns,),
            in_specs=[whole] * count + specs + [column] * len(extra),
            out_specs=column,
        ),
        out_shape=jax.ShapeDtypeStruct((tokens, model), dtype),
        compiler_params=pltpu.CompilerParams(vmem_limit_bytes=40 * 1024 * 1024),
        cost_estimate=pl.CostEstimate(
            flops=2 * tokens * model * feats * count,
            transcendentals=0,
            bytes_accessed=2 * model * feats * count,
        ),
        name="project",
    )(spots, *pieces, *arrays, *extra)


def layer(
    query_map, key_map, value_map, window_mask, tile_radius, dilation_per_tile, rel_bias, out_weight
):
    tile_rows, tile_cols, features_dev = query_map.shape
    half_feats = features_dev // 2
    feats = GROUP_HEADS * HEAD_DIM
    slots = tile_cols + 48
    row_id = lax.axis_index("row")
    parity = row_id % 2
    rows_count = lax.axis_size("row")
    pairs_count = rows_count // 2
    tokens = tile_rows * tile_cols
    head_id = lax.axis_index("head")
    model_half = out_weight.shape[1] // 2

    total_groups = half_feats // feats
    parts = [(array, n) for n in range(total_groups) for array in (key_map, value_map)]
    parts += [(query_map, n) for n in range(total_groups)]
    given = give_half(parity.astype(jnp.int32)[None], parts, feats)
    recv = partner(given)

    mine = jnp.concatenate([tile_radius[0], dilation_per_tile[0], window_mask[0, 0].reshape(-1)])
    others = partner(mine)
    dims = jnp.stack([mine, others])
    base = tables(dims, rel_bias.reshape(rel_bias.shape[0], -1), slots)

    downs = {1: [], 2: [None]}.get(pairs_count, [1, 0])
    lows = [n * feats for n in range(total_groups)]
    *edges, first, second = pack(
        key_map, value_map, recv, 0, feats, downs, lows[:1], [], True, []
    )
    if downs and lows[1:]:
        edges += pack(key_map, value_map, recv, 0, feats, downs, lows[1:], [], False, [second])
    middles = []
    for n in range(total_groups):
        if pairs_count == 2:
            middles.append([row_pair_swap(edges[n])])
        else:
            own = edges[n * len(downs) : (n + 1) * len(downs)]
            middles.append([row_shift(edge, 2 if down else -2) for edge, down in zip(own, downs)])
    row_oks = {1: [lambda r: True], 2: [lambda r: r >= 2, lambda r: r < rows_count - 2]}.get(len(downs), [])
    order = []

    def prepare(n):
        halos, wires = [], [first, second]
        if n == 0:
            for middle, row_ok in zip(middles[n], row_oks):
                outs = pack_halo(middle, order[-1:])
                order.append(outs[1])
                halos.append((middle, *[col_swap_where(wire, odd, row_ok) for odd, wire in enumerate(outs)]))
        else:
            wires = pack(key_map, value_map, recv, lows[n], feats, downs, [], middles[n], True, order[-1:])
            order.append(wires[1])
            halos = [(middle,) for middle in middles[n]]
        sides = [col_swap_where(wire, odd, lambda r: True) for odd, wire in enumerate(wires)]
        return sides, halos

    give = lax.dynamic_slice(out_weight, (parity * half_feats, (1 - head_id) * model_half), (half_feats, model_half))
    far_weight = head_swap(give)
    corner = jnp.stack([parity, head_id]).astype(jnp.int32)

    calls = [(n, tiles) for n in range(total_groups - 1) for tiles in ((0, 1),)]
    calls += [(total_groups - 1, (0,)), (total_groups - 1, (1,))]
    exchanged = []
    ready = [prepare(n) for n in range(min(2, total_groups))]
    for index, (n, tiles) in enumerate(calls):
        sides, halos = ready[n]
        done = attend(
            dims, base, key_map, value_map, query_map, recv, *sides, halos, n > 0, order[-1:],
            lows[n], feats, slots, tiles, 2 * n, 2 * total_groups + n,
        )
        if index == len(calls) - 2:
            far_weights = [far_weight, partner(lax.optimization_barrier((far_weight, done))[0])]
        order.append(done)
        if len(ready) < total_groups:
            ready.append(prepare(len(ready)))
        if 0 in tiles:
            own = done[0]
            exchanged += [(n, 0, own), (n, 2, head_swap(own))]
        if 1 in tiles:
            other = done[-1]
            exchanged += [(n, 1, partner(other)), (n, 3, head_partner(other))]
    exchanged = [(n, source, piece.reshape(tokens, feats)) for n, source, piece in exchanged]
    acc = project(corner, exchanged[:-1], out_weight, far_weights, half_feats, None, jnp.float32)
    acc = project(corner, exchanged[-1:], out_weight, far_weights, half_feats, acc, jnp.bfloat16)
    return acc.reshape(tile_rows, tile_cols, model_half)


def solution(mesh):
    placed = (
        P("row", "col", "head"),
        P("row", "col", "head"),
        P("row", "col", "head"),
        P("row", "col", None, None),
        P("row", "col"),
        P("row", "col"),
        P("head", None, None),
        P("head", None),
    )
    return jax.shard_map(layer, mesh=mesh, in_specs=placed, out_specs=P("row", "col", "head"), check_vma=False)
```

```python
import math

import jax
import jax.numpy as jnp
from jax import lax
from jax.experimental import pallas as pl
from jax.experimental.pallas import tpu as pltpu
from jax.sharding import PartitionSpec as P


HEAD_DIM = 64
RADIUS_MAX = 6
WINDOW = 13
HALO = 18
MASKED = -1e30
GROUP_HEADS = 4
GROUP_ROWS = 3


def row_shift(value, steps):
    count = lax.axis_size("row")
    pairs = [(s, s + steps) for s in range(count) if 0 <= s + steps < count]
    return lax.ppermute(value, "row", pairs)


def col_swap_where(value, odd, row_ok):
    rows, cols = lax.axis_size("row"), lax.axis_size("col")
    pairs = []
    for r in range(rows):
        for c in range(odd, cols - 1, 2):
            if row_ok(r):
                low = r * cols + c
                pairs += [(low, low + 1), (low + 1, low)]
    return lax.ppermute(value, ("row", "col"), pairs)


def partner(value):
    count = lax.axis_size("row")
    return lax.ppermute(value, "row", [(s, s ^ 1) for s in range(count)])


def head_swap(value):
    return lax.ppermute(value, "head", [(0, 1), (1, 0)])


def head_partner(value):
    rows = lax.axis_size("row")
    pairs = [(2 * r + h, 2 * (r ^ 1) + 1 - h) for r in range(rows) for h in range(2)]
    return lax.ppermute(value, ("row", "head"), pairs)


def row_pair_swap(value):
    return lax.ppermute(value, "row", [(s, s ^ 2) for s in range(4)])


def tables_kernel(dims_ref, dims_row_ref, bias_ref, base_ref, *, slots):
    half = bias_ref.shape[0] // 2
    width = base_ref.shape[2]
    parity = lax.axis_index("row") % 2
    bias = jnp.where(parity == 0, bias_ref[:half], bias_ref[half:])
    index = lax.broadcasted_iota(jnp.int32, (1, WINDOW * WINDOW), 1)
    column = lax.broadcasted_iota(jnp.int32, (WINDOW * WINDOW, width), 0)
    lane = lax.broadcasted_iota(jnp.int32, (WINDOW * WINDOW, width), 1)
    for tile in range(2):
        radius, dilation = dims_ref[tile, 0], dims_ref[tile, 1]
        pattern = dims_row_ref[tile : tile + 1, 2:]
        up, side = index // WINDOW - RADIUS_MAX, index % WINDOW - RADIUS_MAX
        used = (jnp.abs(up) <= radius) & (jnp.abs(side) <= radius)
        used = used & ((pattern == 1) | ((up == 0) & (side == 0)))
        value = jnp.where(used, bias, MASKED)
        target = column // WINDOW * slots + (column % WINDOW - RADIUS_MAX) * dilation
        target = jnp.where(target < 0, target + width, target)
        spot = jnp.where(target == lane, 1.0, 0.0)
        placed = jnp.dot(value, spot, precision=lax.Precision.HIGHEST, preferred_element_type=jnp.float32)
        taken = jnp.max(spot, axis=0, keepdims=True)
        base_ref[tile] = jnp.where(taken > 0.0, placed, MASKED)


def tables(dims, bias, slots):
    half = bias.shape[0] // 2
    vmem = pl.BlockSpec(memory_space=pltpu.VMEM)

    def body(*refs):
        tables_kernel(*refs, slots=slots)

    return pl.pallas_call(
        body,
        out_shape=jax.ShapeDtypeStruct((2, half, (WINDOW + GROUP_ROWS) * slots), jnp.float32),
        in_specs=[pl.BlockSpec(memory_space=pltpu.SMEM), vmem, vmem],
        out_specs=vmem,
        name="tables",
    )(dims, dims, bias)


def give_half(parity, parts, feats):
    rows, cols, all_feats = parts[0][0].shape
    per_half = all_feats // 2 // feats
    block = 8

    def body(parity_ref, *refs):
        for n, source in enumerate(refs[:-1]):
            refs[-1][n] = source[...]

    def spec(chunk):
        return pl.BlockSpec((block, cols, feats), lambda n, p: (n, 0, (1 - p[0]) * per_half + chunk))

    return pl.pallas_call(
        body,
        grid_spec=pltpu.PrefetchScalarGridSpec(
            num_scalar_prefetch=1,
            grid=(rows // block,),
            in_specs=[spec(chunk) for _, chunk in parts],
            out_specs=pl.BlockSpec((len(parts), block, cols, feats), lambda n, p: (0, n, 0, 0)),
        ),
        out_shape=jax.ShapeDtypeStruct((len(parts), rows, cols, feats), parts[0][0].dtype),
        name="give_half",
    )(parity, *[array for array, _ in parts])


def place():
    row = lax.axis_index("row")
    return row % 2, row // 2, lax.axis_index("col") % 2


def send_out(sources, targets, sems, swap):
    for flip in range(2):

        @pl.when(swap == flip)
        def _(flip=flip):
            made = [
                pltpu.make_async_copy(source, targets[n ^ flip], sems[n]) for n, source in enumerate(sources)
            ]
            for copy in made:
                copy.start()
            for copy in made:
                copy.wait()


def pack_kernel(key_ref, value_ref, recv_ref, *refs, low, downs, edge_lows, halos, wires):
    edges = len(downs) * len(edge_lows)
    rows, cols = recv_ref.shape[1:3]
    half = key_ref.shape[2] // 2
    middle_refs = refs[:halos]
    out_refs, (right_ref, left_ref, mid_ref, edge_ref, sems) = refs[-5 - edges - 2 * wires : -5], refs[-5:]
    edge_outs, wire_outs = out_refs[:edges], out_refs[edges:]
    feats = right_ref.shape[3]
    parity, pair, col_parity = place()
    spill = HALO - rows
    every = slice(None)

    def source(kv, own, start, *where):
        if own:
            lanes = pl.ds(pl.multiple_of(parity * half + start, feats), feats)
            return (key_ref, value_ref)[kv].at[(*where, lanes)]
        return recv_ref.at[(2 * (start // feats) + kv, *where, every)]

    count = 0
    middles, others = [], []

    def start_copy(begin, target, group):
        nonlocal count
        copy = pltpu.make_async_copy(begin, target, sems.at[count])
        count += 1
        copy.start()
        group.append(copy)

    def columns(begin, part, top):
        height = part.stop - part.start
        for kv in range(2):
            start_copy(begin(kv, slice(cols // 2 - 8, cols // 2 + 8)), mid_ref.at[kv, part], middles)
            body = slice(top, top + height)
            start_copy(begin(kv, slice(cols - 16, cols)), right_ref.at[kv, body], others)
            start_copy(begin(kv, slice(0, 16)), left_ref.at[kv, body], others)

    if wires:
        for n, own in enumerate((True, False)):
            part = slice(n * rows, (n + 1) * rows)
            columns(lambda kv, at, own=own: source(kv, own, low, every, at), part, n * rows)
        for n, middle in enumerate(middle_refs):
            part = slice(2 * rows + n * HALO, 2 * rows + (n + 1) * HALO)
            top = wire_rows(2 * rows) + n * wire_rows(HALO)
            columns(lambda kv, at, middle=middle: middle.at[kv, :, at], part, top)

    def edge_copies(chunk, n, own_near, downward):
        copies = []
        spot = chunk * len(downs) + n
        for kv in range(2):
            far_rows = slice(rows - spill, rows) if downward else slice(0, spill)
            index = count + 4 * spot + 2 * kv
            near, far = edge_ref.at[spot, kv, 0:rows], edge_ref.at[spot, kv, rows:HALO]
            begin = edge_lows[chunk]
            near_from = source(kv, own_near, begin, every, every)
            far_from = source(kv, not own_near, begin, far_rows, every)
            copies.append(pltpu.make_async_copy(near_from, near, sems.at[index]))
            copies.append(pltpu.make_async_copy(far_from, far, sems.at[index + 1]))
        return copies

    for n, down in enumerate(downs if edge_lows else []):
        goes_down = jnp.where(pair == 0, 1, 0) if down is None else down
        code = jnp.where(parity == goes_down, 1, 0) + 2 * goes_down
        for case in range(4):

            @pl.when(code == case)
            def _(n=n, case=case):
                for chunk in range(len(edge_lows)):
                    for copy in edge_copies(chunk, n, bool(case & 1), bool(case & 2)):
                        copy.start()

    def pair_up(first, height, top):
        for kv in range(2):
            if height * 2 % 16:
                for ref in (right_ref, left_ref):
                    ref[kv, top + wire_rows(height) - 1] = jnp.zeros((16, feats), recv_ref.dtype)
            for r in range(height):
                slot = r * 2
                spot = (kv, top + height + slot // 16, slice(slot % 16, slot % 16 + 2))
                right_ref[spot] = mid_ref[kv, first + r, 6:8, :]
                left_ref[spot] = mid_ref[kv, first + r, 8:10, :]

    sent = []
    if edge_lows:
        for chunk in range(len(edge_lows)):
            for n in range(len(downs)):
                for copy in edge_copies(chunk, n, True, True):
                    copy.wait()
        for n in range(edges):
            sent.append(pltpu.make_async_copy(edge_ref.at[n], edge_outs[n], sems.at[count + 4 * edges + n]))
            sent[-1].start()
    if wires:
        for copy in middles:
            copy.wait()
        pair_up(0, 2 * rows, 0)
        for n in range(halos):
            pair_up(2 * rows + n * HALO, HALO, wire_rows(2 * rows) + n * wire_rows(HALO))
        for copy in others:
            copy.wait()
        last = count + 5 * edges
        send_out([right_ref, left_ref], wire_outs, [sems.at[last], sems.at[last + 1]], col_parity)
    for copy in sent:
        copy.wait()


def wire_rows(height):
    return height + -(-height * (HALO - 16) // 16)


def pack(key_map, value_map, recv, low, feats, downs, edge_lows, middles, wires, after):
    _, rows, cols, _ = recv.shape
    edges, halos = len(downs) * len(edge_lows), len(middles)
    hbm = pl.BlockSpec(memory_space=pltpu.HBM)
    height = wire_rows(2 * rows) + halos * wire_rows(HALO)
    wire = jax.ShapeDtypeStruct((2, height, 16, feats), recv.dtype)

    def body(*refs):
        pack_kernel(*refs, low=low, downs=downs, edge_lows=edge_lows, halos=halos, wires=wires)

    return pl.pallas_call(
        body,
        out_shape=[jax.ShapeDtypeStruct((2, HALO, cols, feats), recv.dtype)] * edges + [wire, wire] * wires,
        in_specs=[hbm] * (3 + halos + len(after)),
        out_specs=[hbm] * (edges + 2 * wires),
        scratch_shapes=[
            pltpu.VMEM((2, height, 16, feats), recv.dtype),
            pltpu.VMEM((2, height, 16, feats), recv.dtype),
            pltpu.VMEM((2, 2 * rows + halos * HALO, 16, feats), recv.dtype),
            pltpu.VMEM((max(edges, 1), 2, HALO, cols, feats), recv.dtype),
            pltpu.SemaphoreType.DMA((14 + 6 * halos + 5 * edges,)),
        ],
        compiler_params=pltpu.CompilerParams(vmem_limit_bytes=40 * 1024 * 1024),
        name="pack",
    )(key_map, value_map, recv, *middles, *after)


def pack_halo(middle, after):
    _, rows, cols, feats = middle.shape
    vmem = pl.BlockSpec(memory_space=pltpu.VMEM)
    hbm = pl.BlockSpec(memory_space=pltpu.HBM)
    height = wire_rows(rows)
    tail = height - rows
    wire = jax.ShapeDtypeStruct((2, height, 16, feats), middle.dtype)

    def body(in_ref, *refs):
        first_out, second_out, right_ref, left_ref, sems = refs[-5:]
        for kv in range(2):
            right_ref[kv, 0:rows] = in_ref[kv, :, cols - 16 :, :]
            left_ref[kv, 0:rows] = in_ref[kv, :, 0:16, :]
            for ref in (right_ref, left_ref):
                ref[kv, rows + tail - 1] = jnp.zeros((16, feats), middle.dtype)
            for r in range(rows):
                slot = r * 2
                spot = (kv, rows + slot // 16, slice(slot % 16, slot % 16 + 2))
                right_ref[spot] = in_ref[kv, r, cols - HALO : cols - 16, :]
                left_ref[spot] = in_ref[kv, r, 16:HALO, :]
        send_out([right_ref, left_ref], [first_out, second_out], [sems.at[0], sems.at[1]], place()[2])

    return pl.pallas_call(
        body,
        out_shape=[wire, wire],
        in_specs=[vmem] + [hbm] * len(after),
        out_specs=[hbm, hbm],
        scratch_shapes=[pltpu.VMEM(wire.shape, wire.dtype)] * 2 + [pltpu.SemaphoreType.DMA((2,))],
        compiler_params=pltpu.CompilerParams(vmem_limit_bytes=40 * 1024 * 1024),
        name="pack_halo",
    )(middle, *after)


def attend_kernel(dims_ref, base_ref, *refs, halos, joined, low, tiles, recv_at, query_at):
    key_ref, value_ref, query_ref, recv_ref, side_first, side_second = refs[:6]
    per_halo = 1 if joined else 3
    halo_refs = refs[6 : 6 + per_halo * halos]
    out_ref, slab_ref, q_ref, extra_ref, table_ref, rows_ref, sems = refs[-7:]
    groups, _, slab_rows, slots, feats = slab_ref.shape
    tile_rows, cols = q_ref.shape[2], q_ref.shape[3]
    half = key_ref.shape[2] // 2
    heads = feats // HEAD_DIM
    width = table_ref.shape[1]
    keys = (WINDOW + GROUP_ROWS - 1) * slots
    block = heads * cols
    parity, pair, col_parity = place()
    own_row, other_row = parity * tile_rows, (1 - parity) * tile_rows
    spill, pair_rows = HALO - tile_rows, 2 * tile_rows
    pair_base = pair * pair_rows
    total_rows = tile_rows * lax.axis_size("row")
    total_cols = cols * lax.axis_size("col")
    col_anchor = lax.axis_index("col") * cols
    if halos == 0:
        own_off, spots = 0, []
    elif halos == 1:
        own_off = jnp.where(pair == 0, 0, HALO)
        spots = [(jnp.where(pair == 0, pair_rows, spill), jnp.where(pair == 0, pair_rows + tile_rows, 0))]
    else:
        own_off = HALO
        spots = [(spill, 0), (HALO + pair_rows, HALO + pair_rows + tile_rows)]
    slots_at = [cols + 32 * col_parity, cols + 32 * (1 - col_parity)]
    slots_at = [pl.ds(pl.multiple_of(at, 16), 16) for at in slots_at]
    sides_at = [col_parity, 1 - col_parity]
    extra_slots = slice(cols + 16, cols + 32)
    tail = 2 * tile_rows * 2 // 16
    halo_tail = -(-HALO * 2 // 16)

    def places(n):
        if n < 0:
            return [(own_off + own_row, tile_rows, 0), (own_off + other_row, tile_rows, tile_rows)]
        near, far = spots[n]
        return [(near, tile_rows, 0), (far, HALO - tile_rows, tile_rows)]

    def copies(g):
        own = pl.ds(pl.multiple_of(parity * half + low + g * feats, feats), feats)
        here = pl.ds(pl.multiple_of(g * feats, feats), feats)
        made = []

        def add(source, target):
            made.append(pltpu.make_async_copy(source, target, sems.at[g, len(made)]))

        add(query_ref.at[:, :, own], q_ref.at[g, 0])
        add(recv_ref.at[query_at], q_ref.at[g, 1])
        for kv in range(2):
            slab = slab_ref.at[g, kv]
            add((key_ref, value_ref)[kv].at[:, :, own], slab.at[pl.ds(own_off + own_row, tile_rows), 0:cols])
            add(recv_ref.at[recv_at + kv], slab.at[pl.ds(own_off + other_row, tile_rows), 0:cols])
            for n in range(-1, halos):
                wires, top, height, extra = (side_first, side_second), 0, 2 * tile_rows, 0
                if n >= 0:
                    height, extra = HALO, tail + n * halo_tail
                    middle = halo_refs[per_halo * n]
                    if joined:
                        top = wire_rows(2 * tile_rows) + n * wire_rows(HALO)
                    else:
                        wires = halo_refs[3 * n + 1 : 3 * n + 3]
                for start, count, first in places(n):
                    rows = pl.ds(start, count)
                    if n >= 0:
                        add(middle.at[kv, first : first + count, :, here], slab.at[rows, 0:cols])
                    part = slice(top + first, top + first + count)
                    for wire, at in zip(wires, slots_at):
                        add(wire.at[kv, part, :, here], slab.at[rows, at])
                count = tail if n < 0 else halo_tail
                for side, wire in zip(sides_at, wires):
                    target = extra_ref.at[g, kv, side, extra : extra + count]
                    add(wire.at[kv, top + height : top + height + count, :, here], target)
        return made

    def start_group(g, carry):
        for copy in copies(g):
            copy.start()
        return carry

    lax.fori_loop(0, groups, start_group, 0)

    lane = lax.broadcasted_iota(jnp.int32, (1, width), 1)
    step = jnp.zeros((1, width), jnp.int32)
    for m in range(1, width // slots):
        step = step + jnp.where(lane >= m * slots, 1, 0)
    slot = lane - step * slots
    front_ok = jnp.where((slot < cols + HALO) & (col_anchor + slot < total_cols) & (lane < keys), 1, 0)
    back_ok = jnp.where((slot >= slots - HALO) & (col_anchor + slot >= slots) & (lane < keys), 2, 0)
    ok = jnp.broadcast_to(front_ok + back_ok, (cols, width))
    lane_head = lax.broadcasted_iota(jnp.int32, (cols, feats), 1) // HEAD_DIM
    scale = 1.0 / math.sqrt(HEAD_DIM)

    def fill_extras(g):
        for kv in range(2):
            slab_ref[g, kv, :, extra_slots, :] = jnp.zeros((slab_rows, 16, feats), jnp.bfloat16)
            for n in range(-1, halos):
                origin = 0 if n < 0 else tail + n * halo_tail
                for start, count, first in places(n):
                    for r in range(count):
                        at = (first + r) * 2
                        rows = slice(at % 16, at % 16 + 2)
                        where = origin + at // 16
                        slab_ref[g, kv, start + r, cols + 16 : cols + 18, :] = extra_ref[g, kv, 0, where, rows, :]
                        slab_ref[g, kv, start + r, cols + 30 : cols + 32, :] = extra_ref[g, kv, 1, where, rows, :]

    def fill_table(g, tile):
        for h in range(heads):
            head = low // HEAD_DIM + g * heads + h
            base = jnp.broadcast_to(base_ref[tile, pl.ds(head, 1), :], (cols, width))
            for n in range(GROUP_ROWS):
                front = pltpu.roll(base, n * slots, 1, stride=1, stride_axis=0)
                back = pltpu.roll(base, (n + 1) * slots, 1, stride=1, stride_axis=0)
                row0 = n * block + h * cols
                table_ref[row0 : row0 + cols, :] = jnp.where(
                    ok == 1, front, jnp.where(ok == 2, back, MASKED)
                )

    def one_tile(g, tile):
        dilation = dims_ref[tile, 1]
        tile_row = jnp.where(tile == 0, own_row, other_row)

        def unit(p, carry):
            first = (p // dilation) * (GROUP_ROWS * dilation) + p % dilation
            blocks = []
            for n in range(GROUP_ROWS):
                q_row = q_ref[g, tile, jnp.minimum(first + n * dilation, tile_rows - 1)]
                q_row = q_row.astype(jnp.float32) * scale
                blocks += [jnp.where(lane_head == h, q_row, 0.0).astype(jnp.bfloat16) for h in range(heads)]
            q_block = jnp.concatenate(blocks, axis=0)
            top = tile_row + first - RADIUS_MAX * dilation
            starts = [
                jnp.clip(own_off + top + m * dilation, 0, slab_rows - 1)
                for m in range(WINDOW + GROUP_ROWS - 1)
            ]
            k_rows = jnp.concatenate([slab_ref[g, 0, s] for s in starts], axis=0)
            v_rows = jnp.concatenate([slab_ref[g, 1, s] for s in starts], axis=0)
            scores = lax.dot_general(
                q_block, k_rows, (((1,), (1,)), ((), ())), preferred_element_type=jnp.float32
            )
            key_row = pair_base + top + step * dilation
            outside = jnp.where((key_row >= 0) & (key_row < total_rows), 0.0, MASKED)
            weights, sums = [], []
            for n in range(GROUP_ROWS):
                start = n * slots // 128 * 128
                stop = min(-(-(n + WINDOW) * slots // 128) * 128, keys)
                part = slice(n * block, (n + 1) * block)
                score = scores[part, start:stop] + table_ref[part, start:stop] + outside[:, start:stop]
                peak = jnp.max(score, axis=1, keepdims=True)
                exponent = jnp.exp(score - peak)
                sums.append(jnp.sum(exponent, axis=1, keepdims=True))
                pieces = [exponent.astype(jnp.bfloat16)]
                if start:
                    pieces.insert(0, jnp.zeros((block, start), jnp.bfloat16))
                if stop < keys:
                    pieces.append(jnp.zeros((block, keys - stop), jnp.bfloat16))
                weights.append(jnp.concatenate(pieces, axis=1))
            mixed = jnp.dot(
                jnp.concatenate(weights, axis=0), v_rows, preferred_element_type=jnp.float32
            ) / jnp.concatenate(sums, axis=0)
            for n in range(GROUP_ROWS):
                picked = mixed[n * block : n * block + cols]
                for h in range(1, heads):
                    row0 = n * block + h * cols
                    picked = jnp.where(lane_head == h, mixed[row0 : row0 + cols], picked)
                rows_ref[first + n * dilation] = picked.astype(jnp.bfloat16)
            return carry

        lax.fori_loop(0, -(-tile_rows // GROUP_ROWS), unit, 0, unroll=True)
        out_ref[tile - tiles[0], g] = rows_ref[0:tile_rows]

    def one_group(g, carry):
        fill_table(g, tiles[0])
        for copy in copies(g):
            copy.wait()
        fill_extras(g)

        def tile_step(tile, inner):
            @pl.when(tile > tiles[0])
            def _():
                fill_table(g, tile)

            one_tile(g, tile)
            return inner

        lax.fori_loop(tiles[0], tiles[-1] + 1, tile_step, 0)
        return carry

    lax.fori_loop(0, groups, one_group, 0)


def attend(
    dims, base, key_map, value_map, query_map, recv, first, second, halos, joined, after,
    low, all_feats, slots, tiles, recv_at, query_at,
):
    _, tile_rows, cols, _ = recv.shape
    feats = GROUP_HEADS * HEAD_DIM
    groups = all_feats // feats
    slab_rows = 2 * tile_rows + HALO * len(halos)
    count = len(tiles) * tile_rows * groups * GROUP_HEADS * cols * WINDOW * slots
    hbm = pl.BlockSpec(memory_space=pltpu.HBM)
    vmem = pl.BlockSpec(memory_space=pltpu.VMEM)
    flat = [array for halo in halos for array in halo] + list(after)
    tails = 2 * tile_rows * 2 // 16 + len(halos) * -(-HALO * 2 // 16)

    def body(*refs):
        attend_kernel(*refs, halos=len(halos), joined=joined, low=low, tiles=tiles, recv_at=recv_at, query_at=query_at)

    return pl.pallas_call(
        body,
        out_shape=jax.ShapeDtypeStruct((len(tiles), groups, tile_rows, cols, feats), jnp.bfloat16),
        in_specs=[pl.BlockSpec(memory_space=pltpu.SMEM), vmem] + [hbm] * (6 + len(flat)),
        out_specs=vmem,
        scratch_shapes=[
            pltpu.VMEM((groups, 2, slab_rows, slots, feats), jnp.bfloat16),
            pltpu.VMEM((groups, 2, tile_rows, cols, feats), jnp.bfloat16),
            pltpu.VMEM((groups, 2, 2, tails, 16, feats), jnp.bfloat16),
            pltpu.VMEM((GROUP_ROWS * GROUP_HEADS * cols, base.shape[2]), jnp.float32),
            pltpu.VMEM((tile_rows + 8, cols, feats), jnp.bfloat16),
            pltpu.SemaphoreType.DMA((groups, 2 + 2 * (8 + 8 * len(halos)))),
        ],
        compiler_params=pltpu.CompilerParams(vmem_limit_bytes=48 * 1024 * 1024),
        cost_estimate=pl.CostEstimate(
            flops=count * feats * 4, transcendentals=count, bytes_accessed=4 * groups * slab_rows * slots * feats
        ),
        name="attend",
    )(dims, base, key_map, value_map, query_map, recv, first, second, *flat)


def project(spots, terms, out_weight, far_weights, half_feats, before, dtype):
    tokens, feats = terms[0][2].shape
    model = far_weights[0].shape[1]
    block = model // 2
    per_half = half_feats // feats
    columns = model // block
    whole = pl.BlockSpec((tokens, feats), lambda n, spot: (0, 0))
    column = pl.BlockSpec((tokens, block), lambda n, spot: (0, n))
    specs, arrays, pieces = [], [], []
    for index, source, piece in terms:
        if source < 2:

            def at(n, spot, source=source, index=index):
                who = spot[0] if source == 0 else 1 - spot[0]
                return who * per_half + index, spot[1] * columns + n

            arrays.append(out_weight)
        else:

            def at(n, spot, index=index):
                return index, n

            arrays.append(far_weights[source - 2])
        pieces.append(piece)
        specs.append(pl.BlockSpec((feats, block), at))
    extra = [] if before is None else [before]
    count = len(pieces)

    def body(spot_ref, *refs):
        total = refs[-2][...] if extra else None
        for lhs, rhs in zip(refs[:count], refs[count : 2 * count]):
            term = jnp.dot(lhs[...], rhs[...], preferred_element_type=jnp.float32)
            total = term if total is None else total + term
        refs[-1][...] = total.astype(dtype)

    return pl.pallas_call(
        body,
        grid_spec=pltpu.PrefetchScalarGridSpec(
            num_scalar_prefetch=1,
            grid=(columns,),
            in_specs=[whole] * count + specs + [column] * len(extra),
            out_specs=column,
        ),
        out_shape=jax.ShapeDtypeStruct((tokens, model), dtype),
        compiler_params=pltpu.CompilerParams(vmem_limit_bytes=40 * 1024 * 1024),
        cost_estimate=pl.CostEstimate(
            flops=2 * tokens * model * feats * count,
            transcendentals=0,
            bytes_accessed=2 * model * feats * count,
        ),
        name="project",
    )(spots, *pieces, *arrays, *extra)


def layer(
    query_map, key_map, value_map, window_mask, tile_radius, dilation_per_tile, rel_bias, out_weight
):
    tile_rows, tile_cols, features_dev = query_map.shape
    half_feats = features_dev // 2
    feats = GROUP_HEADS * HEAD_DIM
    slots = tile_cols + 48
    row_id = lax.axis_index("row")
    parity = row_id % 2
    rows_count = lax.axis_size("row")
    pairs_count = rows_count // 2
    tokens = tile_rows * tile_cols
    head_id = lax.axis_index("head")
    model_half = out_weight.shape[1] // 2

    total_groups = half_feats // feats
    parts = [(array, n) for n in range(total_groups) for array in (key_map, value_map)]
    parts += [(query_map, n) for n in range(total_groups)]
    given = give_half(parity.astype(jnp.int32)[None], parts, feats)
    recv = partner(given)

    mine = jnp.concatenate([tile_radius[0], dilation_per_tile[0], window_mask[0, 0].reshape(-1)])
    others = partner(mine)
    dims = jnp.stack([mine, others])
    base = tables(dims, rel_bias.reshape(rel_bias.shape[0], -1), slots)

    downs = {1: [], 2: [None]}.get(pairs_count, [1, 0])
    lows = [n * feats for n in range(total_groups)]
    *edges, first, second = pack(
        key_map, value_map, recv, 0, feats, downs, lows[:1], [], True, []
    )
    own_wires = [[first, second]]
    if downs and lows[1:]:
        *more, first, second = pack(
            key_map, value_map, recv, lows[1], feats, downs, lows[1:], [], True, [second]
        )
        edges += more
        own_wires.append([first, second])
    middles = []
    for n in range(total_groups):
        if pairs_count == 2:
            middles.append([row_pair_swap(edges[n])])
        else:
            own = edges[n * len(downs) : (n + 1) * len(downs)]
            middles.append([row_shift(edge, 2 if down else -2) for edge, down in zip(own, downs)])
    row_oks = {1: [lambda r: True], 2: [lambda r: r >= 2, lambda r: r < rows_count - 2]}.get(len(downs), [])
    order = []

    def prepare(n):
        halos = []
        if n < len(own_wires):
            wires = own_wires[n]
            for middle, row_ok in zip(middles[n], row_oks):
                outs = pack_halo(middle, order[-1:])
                order.append(outs[1])
                halos.append((middle, *[col_swap_where(wire, odd, row_ok) for odd, wire in enumerate(outs)]))
        else:
            wires = pack(key_map, value_map, recv, lows[n], feats, downs, [], middles[n], True, order[-1:])
            order.append(wires[1])
            halos = [(middle,) for middle in middles[n]]
        sides = [col_swap_where(wire, odd, lambda r: True) for odd, wire in enumerate(wires)]
        return sides, halos

    give = lax.dynamic_slice(out_weight, (parity * half_feats, (1 - head_id) * model_half), (half_feats, model_half))
    far_weight = head_swap(give)
    corner = jnp.stack([parity, head_id]).astype(jnp.int32)

    calls = [(n, tiles) for n in range(total_groups - 1) for tiles in ((0, 1),)]
    calls += [(total_groups - 1, (0,)), (total_groups - 1, (1,))]
    exchanged = []
    ready = [prepare(n) for n in range(min(2, total_groups))]
    for index, (n, tiles) in enumerate(calls):
        sides, halos = ready[n]
        done = attend(
            dims, base, key_map, value_map, query_map, recv, *sides, halos, n >= len(own_wires), order[-1:],
            lows[n], feats, slots, tiles, 2 * n, 2 * total_groups + n,
        )
        if index == len(calls) - 2:
            far_weights = [far_weight, partner(lax.optimization_barrier((far_weight, done))[0])]
        order.append(done)
        if len(ready) < total_groups:
            ready.append(prepare(len(ready)))
        if 0 in tiles:
            own = done[0]
            exchanged += [(n, 0, own), (n, 2, head_swap(own))]
        if 1 in tiles:
            other = done[-1]
            exchanged += [(n, 1, partner(other)), (n, 3, head_partner(other))]
    exchanged = [(n, source, piece.reshape(tokens, feats)) for n, source, piece in exchanged]
    acc = project(corner, exchanged[:-1], out_weight, far_weights, half_feats, None, jnp.float32)
    acc = project(corner, exchanged[-1:], out_weight, far_weights, half_feats, acc, jnp.bfloat16)
    return acc.reshape(tile_rows, tile_cols, model_half)


def solution(mesh):
    placed = (
        P("row", "col", "head"),
        P("row", "col", "head"),
        P("row", "col", "head"),
        P("row", "col", None, None),
        P("row", "col"),
        P("row", "col"),
        P("head", None, None),
        P("head", None),
    )
    return jax.shard_map(layer, mesh=mesh, in_specs=placed, out_specs=P("row", "col", "head"), check_vma=False)
```
